32 devices in a mesh: row: 4 (over z), col: 8 (over y, x, core).
Axes of the slice: x: 2, y: 2, z: 4, core: 2. Of those that a mesh axis runs over, the one named last changes fastest.
Arguments:
- eigvecs: bfloat16 [40960, 2048], P('row', 'col'), may hold values from -0.125 to 0.125
- reflectors: bfloat16 [2, 40960, 128], P(None, 'row'), may hold values from -6 to 6
- factors: float32 [2, 128, 128], replicated, may hold values from -0.00024414062 to 0.00024414062
- frequencies: float32 [2048], replicated, may hold values from 0.3 to 3
- region_blocks: int32 [72], P('row'), may hold values from 0 to 319, as said below
Outputs:
- covariance: float32 [9216, 9216], P('row', 'col')
The draws below stay inside these ranges and needn't reach their ends.
Inputs may be any that keep to these rules, and one draw needn't show every extreme that they name: `region_blocks`: the 72 block numbers are distinct and ascending; exactly 18 of them lie in each consecutive run of 80 block numbers.
All inputs are finite; a program needn't handle non-finite values.
Results may differ from the reference program's by a relative error of at most 0.004.
Values may be sent and summed in bfloat16 or wider, within the bound.
A program may use at most 128 MiB of HBM per device.

```python
import math
import jax
import jax.numpy as jnp
from jax import lax

ROWS_DEV = 10240
HB = 128
BLOCK = 128
N = 40960
K = 2048
RBD = 18
N_ROW = 4


def draw_region_blocks(key, part):
    local_blocks = ROWS_DEV // BLOCK
    scores = jax.random.randint(key, (N_ROW, local_blocks), 0, 1 << 20)
    scores = scores * local_blocks + jnp.arange(local_blocks, dtype=jnp.int32)[None, :]
    chosen = lax.top_k(scores, RBD)[1]
    chosen = jnp.sort(chosen, axis=1)
    chosen = chosen + jnp.arange(N_ROW, dtype=jnp.int32)[:, None] * local_blocks
    return chosen.reshape(-1).astype(jnp.int32)


def level_of(key, shape, pieces, low, top_value):
    level = 1.0
    for axis_at, blocks in pieces:
        draws = jax.random.uniform(jax.random.fold_in(jax.random.fold_in(key, 6), axis_at), (blocks,), jnp.float32, low / len(pieces), top_value / len(pieces))
        level = level * jnp.repeat(jnp.exp(draws), shape[axis_at] // blocks).reshape((-1,) + (1,) * (len(shape) - 1 - axis_at))
    return level


def scatter_about(own_key, shape, spread, reach, pieces=(), kind=jnp.bfloat16):
    array = jax.random.normal(own_key, shape, jnp.float32) * spread
    if len(pieces) > 0:
        array = level_of(own_key, shape, pieces, -0.22, 0.18) * array
    return jnp.clip(array, min=-reach, max=reach).astype(kind)


def setup_inputs(seed: int = 0) -> dict:
    seeds = jax.random.split(jax.random.key(seed), 6)
    return {
        "eigvecs": scatter_about(seeds[0], (N, K), K ** -0.5, 0.125, ((0, 4), (1, 8))),
        "reflectors": scatter_about(seeds[1], (2, N, HB), 1.0, 6.0, ((1, 4),)),
        "factors": scatter_about(seeds[2], (2, HB, HB), (HB * HB * N) ** -0.5, 0.00024414062, (), jnp.float32),
        "frequencies": jnp.clip(jnp.exp(jax.random.uniform(seeds[3], (K,), jnp.float32, math.log(0.3), math.log(3.0))), 0.3, 3.0),
        "region_blocks": draw_region_blocks(jax.random.fold_in(seeds[5], 71), 0),
    }


def contract_rows(left, right):
    return lax.dot_general(left, right, (((0,), (0,)), ((), ())), preferred_element_type=jnp.float32)


def reference(eigvecs, reflectors, factors, frequencies, region_blocks):
    first_block = reflectors[0]
    second_block = reflectors[1]
    first_factor = jnp.triu(factors[0])
    second_factor = jnp.triu(factors[1])
    highest = lax.Precision.HIGHEST
    second_proj = contract_rows(second_block, eigvecs)
    second_apply = jnp.dot(second_factor, second_proj, precision=highest).astype(jnp.bfloat16)
    cross = contract_rows(first_block, second_block)
    first_proj = contract_rows(first_block, eigvecs) - jnp.dot(cross, second_apply.astype(jnp.float32), precision=highest)
    first_apply = jnp.dot(first_factor, first_proj, precision=highest).astype(jnp.bfloat16)
    offsets = jnp.arange(BLOCK, dtype=jnp.int32)
    rows = (region_blocks.astype(jnp.int32)[:, None] * BLOCK + offsets[None, :]).reshape(-1)
    region = eigvecs[rows].astype(jnp.float32)
    region = region - jnp.dot(second_block[rows], second_apply, preferred_element_type=jnp.float32)
    region = region - jnp.dot(first_block[rows], first_apply, preferred_element_type=jnp.float32)
    region = region.astype(jnp.bfloat16)
    weight = 1.0 / jnp.tanh(frequencies / 2.0) / (2.0 * frequencies)
    scaled = (region.astype(jnp.float32) * weight[None, :]).astype(jnp.bfloat16)
    return lax.dot_general(scaled, region, (((1,), (1,)), ((), ())), preferred_element_type=jnp.float32)
```

```python
import functools

import jax
import jax.numpy as jnp
from jax import lax
from jax.experimental import pallas as pl
from jax.experimental.pallas import tpu as pltpu
from jax.sharding import PartitionSpec as P

BLOCK = 128
MESH = pl.DeviceIdType.MESH
SUB = 8


def contract_rows(left, right):
    return lax.dot_general(
        left, right, (((0,), (0,)), ((), ())), preferred_element_type=jnp.float32
    )


def contract_cols(left, right):
    return lax.dot_general(
        left, right, (((1,), (1,)), ((), ())), preferred_element_type=jnp.float32
    )


def exchange_kernel(
    n_row, sub, x_ref, a_ref, b_ref, half_buf,
    own_sem, send_plane, send_sib, recv_a, send_z, recv_b, fill_sem,
):
    r = lax.axis_index("row")
    c = lax.axis_index("col")
    k = c // 2
    h = lax.rem(c, 2)
    o = 1 - h
    sib = 2 * k + o
    rows, cols = x_ref.shape
    step = rows // sub
    hsub = sub // 2
    half = rows // 2
    has_up = (r < n_row - 1).astype(jnp.int32)
    has_dn = (r > 0).astype(jnp.int32)

    barrier = pltpu.get_barrier_semaphore()

    def greet(row, col):
        pl.semaphore_signal(barrier, inc=1, device_id=(row, col), device_id_type=MESH)

    greet(r, sib)
    for d in range(1, n_row):
        greet(r, 2 * (k ^ d) + h)

    @pl.when(r < n_row - 1)
    def _():
        greet(r + 1, c)

    @pl.when(r > 0)
    def _():
        greet(r - 1, c)

    pl.semaphore_wait(barrier, n_row + has_up + has_dn)

    def piece_cols(d, side):
        owner = 2 * (k ^ d) + (h if side == 0 else o)
        return pl.ds(pl.multiple_of(owner * cols, cols), cols)

    def a_at(d, side, s):
        return a_ref.at[pl.ds(s * step, step), piece_cols(d, side)]

    def plane_copy(d, s):
        return pltpu.make_async_remote_copy(
            src_ref=x_ref.at[pl.ds(s * step, step), :],
            dst_ref=a_ref.at[pl.ds(s * step, step), piece_cols(0, 0)],
            send_sem=send_plane.at[d, s], recv_sem=recv_a.at[d, 0, s],
            device_id=(r, 2 * (k ^ d) + h), device_id_type=MESH,
        )

    def sib_copy(d, s):
        src = x_ref.at[pl.ds(s * step, step), :] if d == 0 else a_at(d, 0, s)
        return pltpu.make_async_remote_copy(
            src_ref=src, dst_ref=a_at(d, 0, s),
            send_sem=send_sib.at[d, s], recv_sem=recv_a.at[d, 1, s],
            device_id=(r, sib), device_id_type=MESH,
        )

    def half_rows(t):
        return pl.ds(pl.multiple_of(h * half + t * step, step), step)

    def z_copy(src, way, target, d, side, t):
        return pltpu.make_async_remote_copy(
            src_ref=src,
            dst_ref=b_ref.at[pl.ds(t * step, step), piece_cols(d, side)],
            send_sem=send_z.at[way, d, side, t], recv_sem=recv_b.at[d, side, t],
            device_id=(target, c), device_id_type=MESH,
        )

    def from_source(way, target, d, side, t):
        if d == 0 and side == 0:
            src = x_ref.at[half_rows(t), :]
        else:
            src = a_ref.at[half_rows(t), piece_cols(d, side)]
        return z_copy(src, way, target, d, side, t)

    def relay(way, target, d, side, t):
        src = b_ref.at[pl.ds(t * step, step), piece_cols(d, side)]
        return z_copy(src, way, target, d, side, t)

    own = pltpu.make_async_copy(x_ref, a_ref.at[:, piece_cols(0, 0)], own_sem)
    own.start()
    for s in range(sub):
        sib_copy(0, s).start()
    for d in range(1, n_row):
        for s in range(sub):
            plane_copy(d, s).start()

    arrivals = [(d, s) for d in range(1, n_row) for s in range(sub)]
    parts = [(d, side, t) for d in range(n_row) for side in (0, 1) for t in range(hsub)]

    def take_a(d, s):
        plane_copy(d, s).wait_recv()
        sib_copy(d, s).start()

    at_source = r == k
    above = r > k
    below = r < k

    @pl.when(at_source)
    def _():
        def push(d, side, t):
            @pl.when(r < n_row - 1)
            def _():
                from_source(0, r + 1, d, side, t).start()

            @pl.when(r > 0)
            def _():
                from_source(1, r - 1, d, side, t).start()

        for d in range(n_row):
            if d:
                for s in range(sub):
                    take_a(d, s)
            else:
                for t in range(hsub):
                    push(d, 0, t)
            for s in range(sub):
                sib_copy(d, s).wait_recv()
            for side in (0, 1) if d else (1,):
                for t in range(hsub):
                    push(d, side, t)
        own.wait()
        fill = pltpu.make_async_copy(
            a_ref.at[pl.ds(pl.multiple_of(h * half, half), half), :], half_buf, fill_sem
        )
        fill.start()
        fill.wait()
        out = pltpu.make_async_copy(half_buf, b_ref, fill_sem)
        out.start()
        out.wait()

    @pl.when(jnp.logical_not(at_source))
    def _():
        for i, (d, side, t) in enumerate(parts):
            if i < len(arrivals):
                take_a(*arrivals[i])
            relay(0, r, d, side, t).wait_recv()

            @pl.when(above & (r < n_row - 1))
            def _():
                relay(0, r + 1, d, side, t).start()

            @pl.when(below & (r > 0))
            def _():
                relay(1, r - 1, d, side, t).start()

        for d, s in arrivals[len(parts):]:
            take_a(d, s)
        for d in range(n_row):
            for s in range(sub):
                sib_copy(d, s).wait_recv()
        own.wait()

    for d in range(n_row):
        for s in range(sub):
            sib_copy(d, s).wait_send()
            if d:
                plane_copy(d, s).wait_send()
    for d, side, t in parts:
        @pl.when((r >= k) & (r < n_row - 1))
        def _():
            relay(0, r, d, side, t).wait_send()

        @pl.when((r <= k) & (r > 0))
        def _():
            relay(1, r, d, side, t).wait_send()


def exchange(x, n_row):
    rows, cols = x.shape
    n_col = 2 * n_row
    sub = SUB if n_row <= 4 else SUB // 2
    hsub = sub // 2
    dma = pltpu.SemaphoreType.DMA
    return pl.pallas_call(
        functools.partial(exchange_kernel, n_row, sub),
        out_shape=(
            jax.ShapeDtypeStruct((rows, cols * n_col), x.dtype),
            jax.ShapeDtypeStruct((rows // 2, cols * n_col), x.dtype),
        ),
        in_specs=[pl.BlockSpec(memory_space=pltpu.VMEM)],
        out_specs=(pl.BlockSpec(memory_space=pl.ANY),) * 2,
        scratch_shapes=[
            pltpu.VMEM((rows // 2, cols * n_col), x.dtype),
            dma,
            dma((n_row, sub)),
            dma((n_row, sub)),
            dma((n_row, 2, sub)),
            dma((2, n_row, 2, hsub)),
            dma((n_row, 2, hsub)),
            dma,
        ],
        compiler_params=pltpu.CompilerParams(collective_id=0, has_side_effects=True),
        name="exchange",
    )(x)


def per_device(n_row, eigvecs, reflectors, factors, frequencies, region_blocks):
    highest = lax.Precision.HIGHEST
    first_block = reflectors[0]
    second_block = reflectors[1]
    first_factor = jnp.triu(factors[0])
    second_factor = jnp.triu(factors[1])
    second_local = contract_rows(second_block, eigvecs)
    first_local = contract_rows(first_block, eigvecs)
    cross_local = contract_rows(first_block, second_block)
    second_proj, first_part, cross = lax.psum((second_local, first_local, cross_local), "row")
    second_apply = jnp.dot(second_factor, second_proj, precision=highest).astype(jnp.bfloat16)
    first_proj = first_part - jnp.dot(cross, second_apply.astype(jnp.float32), precision=highest)
    first_apply = jnp.dot(first_factor, first_proj, precision=highest).astype(jnp.bfloat16)
    local_blocks = eigvecs.shape[0] // BLOCK
    columns = eigvecs.shape[1]
    width = reflectors.shape[2]
    local_index = region_blocks - lax.axis_index("row") * local_blocks
    picked_vecs = jnp.take(
        eigvecs.reshape(local_blocks, BLOCK, columns), local_index, axis=0
    ).reshape(-1, columns)
    picked_refl = jnp.take(
        reflectors.reshape(2, local_blocks, BLOCK, width), local_index, axis=1
    ).reshape(2, -1, width)
    region = picked_vecs.astype(jnp.float32)
    region = region - jnp.dot(picked_refl[1], second_apply, preferred_element_type=jnp.float32)
    region = region - jnp.dot(picked_refl[0], first_apply, preferred_element_type=jnp.float32)
    region = region.astype(jnp.bfloat16)
    weight = 1.0 / jnp.tanh(frequencies / 2.0) / (2.0 * frequencies)
    mine, partner = exchange(region, n_row)
    scaled = (mine.astype(jnp.float32) * weight[None, :]).astype(jnp.bfloat16)
    return contract_cols(scaled, partner)


def solution(mesh):
    return jax.shard_map(
        functools.partial(per_device, mesh.shape["row"]),
        mesh=mesh,
        in_specs=(P("row", "col"), P(None, "row", None), P(), P(), P("row")),
        out_specs=P("row", "col"),
        check_vma=False,
    )
```

```python
import functools

import jax
import jax.numpy as jnp
from jax import lax
from jax.experimental import pallas as pl
from jax.experimental.pallas import tpu as pltpu
from jax.sharding import PartitionSpec as P

BLOCK = 128
MESH = pl.DeviceIdType.MESH
SUB = 8


def contract_rows(left, right):
    return lax.dot_general(
        left, right, (((0,), (0,)), ((), ())), preferred_element_type=jnp.float32
    )


def contract_cols(left, right):
    return lax.dot_general(
        left, right, (((1,), (1,)), ((), ())), preferred_element_type=jnp.float32
    )


def exchange_kernel(
    n_row, sub, x_ref, a_ref, b_ref, half_buf,
    own_sem, send_plane, send_sib, recv_a, send_z, recv_b, fill_sem,
):
    r = lax.axis_index("row")
    c = lax.axis_index("col")
    k = c // 2
    h = lax.rem(c, 2)
    o = 1 - h
    sib = 2 * k + o
    rows, cols = x_ref.shape
    step = rows // sub
    hsub = sub // 2
    half = rows // 2
    has_up = (r < n_row - 1).astype(jnp.int32)
    has_dn = (r > 0).astype(jnp.int32)

    barrier = pltpu.get_barrier_semaphore()

    def greet(row, col):
        pl.semaphore_signal(barrier, inc=1, device_id=(row, col), device_id_type=MESH)

    greet(r, sib)
    for d in range(1, n_row):
        greet(r, 2 * (k ^ d) + h)

    @pl.when(r < n_row - 1)
    def _():
        greet(r + 1, c)

    @pl.when(r > 0)
    def _():
        greet(r - 1, c)

    pl.semaphore_wait(barrier, n_row + has_up + has_dn)

    def piece_cols(d, side):
        owner = 2 * (k ^ d) + (h if side == 0 else o)
        return pl.ds(pl.multiple_of(owner * cols, cols), cols)

    def a_at(d, side, s):
        return a_ref.at[pl.ds(s * step, step), piece_cols(d, side)]

    def plane_copy(d, s):
        return pltpu.make_async_remote_copy(
            src_ref=x_ref.at[pl.ds(s * step, step), :],
            dst_ref=a_ref.at[pl.ds(s * step, step), piece_cols(0, 0)],
            send_sem=send_plane.at[d, s], recv_sem=recv_a.at[d, 0, s],
            device_id=(r, 2 * (k ^ d) + h), device_id_type=MESH,
        )

    def sib_copy(d, s):
        src = x_ref.at[pl.ds(s * step, step), :] if d == 0 else a_at(d, 0, s)
        return pltpu.make_async_remote_copy(
            src_ref=src, dst_ref=a_at(d, 0, s),
            send_sem=send_sib.at[d, s], recv_sem=recv_a.at[d, 1, s],
            device_id=(r, sib), device_id_type=MESH,
        )

    def half_rows(t):
        return pl.ds(pl.multiple_of(h * half + t * step, step), step)

    def z_copy(src, way, target, d, side, t):
        return pltpu.make_async_remote_copy(
            src_ref=src,
            dst_ref=b_ref.at[pl.ds(t * step, step), piece_cols(d, side)],
            send_sem=send_z.at[way, d, side, t], recv_sem=recv_b.at[d, side, t],
            device_id=(target, c), device_id_type=MESH,
        )

    def from_source(way, target, d, side, t):
        if d == 0 and side == 0:
            src = x_ref.at[half_rows(t), :]
        else:
            src = a_ref.at[half_rows(t), piece_cols(d, side)]
        return z_copy(src, way, target, d, side, t)

    def relay(way, target, d, side, t):
        src = b_ref.at[pl.ds(t * step, step), piece_cols(d, side)]
        return z_copy(src, way, target, d, side, t)

    own = pltpu.make_async_copy(x_ref, a_ref.at[:, piece_cols(0, 0)], own_sem)
    own.start()
    for s in range(sub):
        sib_copy(0, s).start()
    for d in range(1, n_row):
        for s in range(sub):
            plane_copy(d, s).start()

    arrivals = [(d, s) for d in range(1, n_row) for s in range(sub)]
    parts = [(d, side, t) for d in range(n_row) for side in (0, 1) for t in range(hsub)]

    def take_a(d, s):
        plane_copy(d, s).wait_recv()
        sib_copy(d, s).start()

    at_source = r == k
    above = r > k
    below = r < k

    @pl.when(at_source)
    def _():
        def push(d, side, t):
            @pl.when(r < n_row - 1)
            def _():
                from_source(0, r + 1, d, side, t).start()

            @pl.when(r > 0)
            def _():
                from_source(1, r - 1, d, side, t).start()

        for d in range(n_row):
            if d:
                for s in range(sub):
                    take_a(d, s)
            else:
                for t in range(hsub):
                    push(d, 0, t)
            for s in range(sub):
                sib_copy(d, s).wait_recv()
            for side in (0, 1) if d else (1,):
                for t in range(hsub):
                    push(d, side, t)
        own.wait()
        fill = pltpu.make_async_copy(
            a_ref.at[pl.ds(pl.multiple_of(h * half, half), half), :], half_buf, fill_sem
        )
        fill.start()
        fill.wait()
        out = pltpu.make_async_copy(half_buf, b_ref, fill_sem)
        out.start()
        out.wait()

    @pl.when(jnp.logical_not(at_source))
    def _():
        for i, (d, side, t) in enumerate(parts):
            if i < len(arrivals):
                take_a(*arrivals[i])
            relay(0, r, d, side, t).wait_recv()

            @pl.when(above & (r < n_row - 1))
            def _():
                relay(0, r + 1, d, side, t).start()

            @pl.when(below & (r > 0))
            def _():
                relay(1, r - 1, d, side, t).start()

        for d, s in arrivals[len(parts):]:
            take_a(d, s)
        for d in range(n_row):
            for s in range(sub):
                sib_copy(d, s).wait_recv()
        own.wait()

    for d in range(n_row):
        for s in range(sub):
            sib_copy(d, s).wait_send()
            if d:
                plane_copy(d, s).wait_send()
    for d, side, t in parts:
        @pl.when((r >= k) & (r < n_row - 1))
        def _():
            relay(0, r, d, side, t).wait_send()

        @pl.when((r <= k) & (r > 0))
        def _():
            relay(1, r, d, side, t).wait_send()


def exchange(x, n_row):
    rows, cols = x.shape
    n_col = 2 * n_row
    sub = SUB if n_row <= 4 else SUB // 2
    hsub = sub // 2
    dma = pltpu.SemaphoreType.DMA
    return pl.pallas_call(
        functools.partial(exchange_kernel, n_row, sub),
        out_shape=(
            jax.ShapeDtypeStruct((rows, cols * n_col), x.dtype),
            jax.ShapeDtypeStruct((rows // 2, cols * n_col), x.dtype),
        ),
        in_specs=[pl.BlockSpec(memory_space=pltpu.VMEM)],
        out_specs=(pl.BlockSpec(memory_space=pl.ANY),) * 2,
        scratch_shapes=[
            pltpu.VMEM((rows // 2, cols * n_col), x.dtype),
            dma,
            dma((n_row, sub)),
            dma((n_row, sub)),
            dma((n_row, 2, sub)),
            dma((2, n_row, 2, hsub)),
            dma((n_row, 2, hsub)),
            dma,
        ],
        compiler_params=pltpu.CompilerParams(collective_id=0, has_side_effects=True),
        name="exchange",
    )(x)


def project_kernel(
    n_row, w_ref, g_ref, t_ref, p_ref,
    w_in, g_in, w_sum, g_sum, w_full, g_full, send_1, recv_1, send_2, recv_2,
):
    r = lax.axis_index("row")
    c = lax.axis_index("col")
    barrier = pltpu.get_barrier_semaphore()
    for d in range(1, n_row):
        pl.semaphore_signal(barrier, inc=1, device_id=(r ^ d, c), device_id_type=MESH)
    pl.semaphore_wait(barrier, n_row - 1)
    pairs = ((w_ref, w_in, w_sum, w_full), (g_ref, g_in, g_sum, g_full))

    def part(array, owner):
        size = array.shape[0] // n_row
        return pl.ds(pl.multiple_of(owner * size, size), size)

    def scatter(d, i):
        array, landing, _, _ = pairs[i]
        return pltpu.make_async_remote_copy(
            src_ref=array.at[part(array, r ^ d), :], dst_ref=landing.at[d],
            send_sem=send_1.at[d, i], recv_sem=recv_1.at[d, i],
            device_id=(r ^ d, c), device_id_type=MESH,
        )

    def spread(d, i):
        array, _, total, full = pairs[i]
        return pltpu.make_async_remote_copy(
            src_ref=total, dst_ref=full.at[part(array, r), :],
            send_sem=send_2.at[d, i], recv_sem=recv_2.at[d, i],
            device_id=(r ^ d, c), device_id_type=MESH,
        )

    every = [(d, i) for d in range(1, n_row) for i in (1, 0)]
    for d, i in every:
        scatter(d, i).start()
    for d, i in every:
        scatter(d, i).wait_recv()
    for i in (1, 0):
        array, landing, total, full = pairs[i]
        value = array[part(array, r), :]
        for d in range(1, n_row):
            value = value + landing[d]
        total[...] = value
    for i in (1, 0):
        array, _, total, full = pairs[i]
        full[part(array, r), :] = total[...]
    for d, i in every:
        spread(d, i).start()
    for d, i in every:
        spread(d, i).wait_recv()
    highest = lax.Precision.HIGHEST
    width = g_ref.shape[0]
    second = jnp.dot(
        t_ref[1], w_full[width:, :], precision=highest, preferred_element_type=jnp.float32
    ).astype(jnp.bfloat16)
    first = w_full[:width, :] - jnp.dot(
        g_full[...], second.astype(jnp.float32),
        precision=highest, preferred_element_type=jnp.float32,
    )
    first = jnp.dot(t_ref[0], first, precision=highest, preferred_element_type=jnp.float32)
    p_ref[0] = first.astype(jnp.bfloat16)
    p_ref[1] = second
    for d, i in every:
        scatter(d, i).wait_send()
        spread(d, i).wait_send()


def project(w, g, factors, n_row):
    dma = pltpu.SemaphoreType.DMA((n_row, 2))
    width, columns = g.shape[0], w.shape[1]
    vmem = pl.BlockSpec(memory_space=pltpu.VMEM)

    def landing(array):
        return pltpu.VMEM((n_row, array.shape[0] // n_row, array.shape[1]), jnp.float32)

    def total(array):
        return pltpu.VMEM((array.shape[0] // n_row, array.shape[1]), jnp.float32)

    return pl.pallas_call(
        functools.partial(project_kernel, n_row),
        out_shape=jax.ShapeDtypeStruct((2, width, columns), jnp.bfloat16),
        in_specs=[vmem] * 3,
        out_specs=vmem,
        scratch_shapes=[
            landing(w), landing(g), total(w), total(g),
            pltpu.VMEM(w.shape, jnp.float32), pltpu.VMEM(g.shape, jnp.float32),
            dma, dma, dma, dma,
        ],
        compiler_params=pltpu.CompilerParams(collective_id=1, has_side_effects=True),
        name="project",
    )(w, g, factors)


def region_kernel(index_ref, p_ref, vecs_ref, refl_ref, out_ref, vecs, refl, sems):
    count = vecs.shape[0]

    def copies(b):
        at = index_ref[b]
        return (
            pltpu.make_async_copy(vecs_ref.at[at], vecs.at[b], sems.at[b, 0]),
            pltpu.make_async_copy(refl_ref.at[0, at], refl.at[0, b], sems.at[b, 1]),
            pltpu.make_async_copy(refl_ref.at[1, at], refl.at[1, b], sems.at[b, 2]),
        )

    for b in range(count):
        for copy in copies(b):
            copy.start()
    for b in range(count):
        for copy in copies(b):
            copy.wait()
        value = vecs[b].astype(jnp.float32)
        value = value - jnp.dot(refl[1, b], p_ref[1], preferred_element_type=jnp.float32)
        value = value - jnp.dot(refl[0, b], p_ref[0], preferred_element_type=jnp.float32)
        out_ref[b] = value.astype(out_ref.dtype)


def region_rows(index, applied, vecs, refl):
    count = index.shape[0]
    columns, width = vecs.shape[2], refl.shape[3]
    vmem = pl.BlockSpec(memory_space=pltpu.VMEM)
    hbm = pl.BlockSpec(memory_space=pl.ANY)
    return pl.pallas_call(
        region_kernel,
        out_shape=jax.ShapeDtypeStruct((count, BLOCK, columns), vecs.dtype),
        in_specs=[pl.BlockSpec(memory_space=pltpu.SMEM), vmem, hbm, hbm],
        out_specs=vmem,
        scratch_shapes=[
            pltpu.VMEM((count, BLOCK, columns), vecs.dtype),
            pltpu.VMEM((2, count, BLOCK, width), refl.dtype),
            pltpu.SemaphoreType.DMA((count, 3)),
        ],
        name="region",
    )(index, applied, vecs, refl)


def per_device(n_row, eigvecs, reflectors, factors, frequencies, region_blocks):
    columns = eigvecs.shape[1]
    width = reflectors.shape[2]
    local = lax.dot_general(
        reflectors, eigvecs, (((1,), (0,)), ((), ())), preferred_element_type=jnp.float32
    ).reshape(2 * width, columns)
    cross_local = contract_rows(reflectors[0], reflectors[1])
    applied = project(local, cross_local, jnp.triu(factors), n_row)
    local_blocks = eigvecs.shape[0] // BLOCK
    local_index = region_blocks - lax.axis_index("row") * local_blocks
    region = region_rows(
        local_index,
        applied,
        eigvecs.reshape(local_blocks, BLOCK, columns),
        reflectors.reshape(2, local_blocks, BLOCK, width),
    ).reshape(-1, columns)
    weight = 1.0 / jnp.tanh(frequencies / 2.0) / (2.0 * frequencies)
    mine, partner = exchange(region, n_row)
    scaled = (mine.astype(jnp.float32) * weight[None, :]).astype(jnp.bfloat16)
    return contract_cols(scaled, partner)


def solution(mesh):
    return jax.shard_map(
        functools.partial(per_device, mesh.shape["row"]),
        mesh=mesh,
        in_specs=(P("row", "col"), P(None, "row", None), P(), P(), P("row")),
        out_specs=P("row", "col"),
        check_vma=False,
    )
```

```python
import functools

import jax
import jax.numpy as jnp
from jax import lax
from jax.experimental import pallas as pl
from jax.experimental.pallas import tpu as pltpu
from jax.sharding import PartitionSpec as P

BLOCK = 128
MESH = pl.DeviceIdType.MESH
SUB = 12


def contract_rows(left, right):
    return lax.dot_general(
        left, right, (((0,), (0,)), ((), ())), preferred_element_type=jnp.float32
    )


def contract_cols(left, right):
    return lax.dot_general(
        left, right, (((1,), (1,)), ((), ())), preferred_element_type=jnp.float32
    )


def exchange_kernel(
    n_row, sub, x_ref, a_ref, b_ref, half_buf,
    own_sem, send_plane, send_sib, recv_a, send_z, recv_b, fill_sem,
):
    r = lax.axis_index("row")
    c = lax.axis_index("col")
    k = c // 2
    h = lax.rem(c, 2)
    o = 1 - h
    sib = 2 * k + o
    rows, cols = x_ref.shape
    step = rows // sub
    hsub = sub // 2
    half = rows // 2
    has_up = (r < n_row - 1).astype(jnp.int32)
    has_dn = (r > 0).astype(jnp.int32)

    barrier = pltpu.get_barrier_semaphore()

    def greet(row, col):
        pl.semaphore_signal(barrier, inc=1, device_id=(row, col), device_id_type=MESH)

    greet(r, sib)
    for d in range(1, n_row):
        greet(r, 2 * (k ^ d) + h)

    @pl.when(r < n_row - 1)
    def _():
        greet(r + 1, c)

    @pl.when(r > 0)
    def _():
        greet(r - 1, c)

    pl.semaphore_wait(barrier, n_row + has_up + has_dn)

    def piece_cols(d, side):
        owner = 2 * (k ^ d) + (h if side == 0 else o)
        return pl.ds(pl.multiple_of(owner * cols, cols), cols)

    def a_at(d, side, s):
        return a_ref.at[pl.ds(s * step, step), piece_cols(d, side)]

    def plane_copy(d, s):
        return pltpu.make_async_remote_copy(
            src_ref=x_ref.at[pl.ds(s * step, step), :],
            dst_ref=a_ref.at[pl.ds(s * step, step), piece_cols(0, 0)],
            send_sem=send_plane.at[d, s], recv_sem=recv_a.at[d, 0, s],
            device_id=(r, 2 * (k ^ d) + h), device_id_type=MESH,
        )

    def sib_copy(d, s):
        src = x_ref.at[pl.ds(s * step, step), :] if d == 0 else a_at(d, 0, s)
        return pltpu.make_async_remote_copy(
            src_ref=src, dst_ref=a_at(d, 0, s),
            send_sem=send_sib.at[d, s], recv_sem=recv_a.at[d, 1, s],
            device_id=(r, sib), device_id_type=MESH,
        )

    def half_rows(t):
        return pl.ds(pl.multiple_of(h * half + t * step, step), step)

    def z_copy(src, way, target, d, side, t):
        return pltpu.make_async_remote_copy(
            src_ref=src,
            dst_ref=b_ref.at[pl.ds(t * step, step), piece_cols(d, side)],
            send_sem=send_z.at[way, d, side, t], recv_sem=recv_b.at[d, side, t],
            device_id=(target, c), device_id_type=MESH,
        )

    def from_source(way, target, d, side, t):
        if d == 0 and side == 0:
            src = x_ref.at[half_rows(t), :]
        else:
            src = a_ref.at[half_rows(t), piece_cols(d, side)]
        return z_copy(src, way, target, d, side, t)

    def relay(way, target, d, side, t):
        src = b_ref.at[pl.ds(t * step, step), piece_cols(d, side)]
        return z_copy(src, way, target, d, side, t)

    own = pltpu.make_async_copy(x_ref, a_ref.at[:, piece_cols(0, 0)], own_sem)
    own.start()
    for s in range(sub):
        sib_copy(0, s).start()
    for d in range(1, n_row):
        for s in range(sub):
            plane_copy(d, s).start()

    arrivals = [(d, s) for d in range(1, n_row) for s in range(sub)]
    parts = [(d, side, t) for d in range(n_row) for side in (0, 1) for t in range(hsub)]

    def take_a(d, s):
        plane_copy(d, s).wait_recv()
        sib_copy(d, s).start()

    at_source = r == k
    above = r > k
    below = r < k

    @pl.when(at_source)
    def _():
        def push(d, side, t):
            @pl.when(r < n_row - 1)
            def _():
                from_source(0, r + 1, d, side, t).start()

            @pl.when(r > 0)
            def _():
                from_source(1, r - 1, d, side, t).start()

        for d in range(n_row):
            if d:
                for s in range(sub):
                    take_a(d, s)
            else:
                for t in range(hsub):
                    push(d, 0, t)
            for s in range(sub):
                sib_copy(d, s).wait_recv()
            for side in (0, 1) if d else (1,):
                for t in range(hsub):
                    push(d, side, t)
        own.wait()
        fill = pltpu.make_async_copy(
            a_ref.at[pl.ds(pl.multiple_of(h * half, half), half), :], half_buf, fill_sem
        )
        fill.start()
        fill.wait()
        out = pltpu.make_async_copy(half_buf, b_ref, fill_sem)
        out.start()
        out.wait()

    @pl.when(jnp.logical_not(at_source))
    def _():
        for i, (d, side, t) in enumerate(parts):
            if i < len(arrivals):
                take_a(*arrivals[i])
            relay(0, r, d, side, t).wait_recv()

            @pl.when(above & (r < n_row - 1))
            def _():
                relay(0, r + 1, d, side, t).start()

            @pl.when(below & (r > 0))
            def _():
                relay(1, r - 1, d, side, t).start()

        for d, s in arrivals[len(parts):]:
            take_a(d, s)
        for d in range(n_row):
            for s in range(sub):
                sib_copy(d, s).wait_recv()
        own.wait()

    for d in range(n_row):
        for s in range(sub):
            sib_copy(d, s).wait_send()
            if d:
                plane_copy(d, s).wait_send()
    for d, side, t in parts:
        @pl.when((r >= k) & (r < n_row - 1))
        def _():
            relay(0, r, d, side, t).wait_send()

        @pl.when((r <= k) & (r > 0))
        def _():
            relay(1, r, d, side, t).wait_send()


def exchange(x, n_row):
    rows, cols = x.shape
    n_col = 2 * n_row
    sub = SUB if n_row <= 4 else SUB // 2
    hsub = sub // 2
    dma = pltpu.SemaphoreType.DMA
    return pl.pallas_call(
        functools.partial(exchange_kernel, n_row, sub),
        out_shape=(
            jax.ShapeDtypeStruct((rows, cols * n_col), x.dtype),
            jax.ShapeDtypeStruct((rows // 2, cols * n_col), x.dtype),
        ),
        in_specs=[pl.BlockSpec(memory_space=pltpu.VMEM)],
        out_specs=(pl.BlockSpec(memory_space=pl.ANY),) * 2,
        scratch_shapes=[
            pltpu.VMEM((rows // 2, cols * n_col), x.dtype),
            dma,
            dma((n_row, sub)),
            dma((n_row, sub)),
            dma((n_row, 2, sub)),
            dma((2, n_row, 2, hsub)),
            dma((n_row, 2, hsub)),
            dma,
        ],
        compiler_params=pltpu.CompilerParams(collective_id=0, has_side_effects=True),
        name="exchange",
    )(x)


def project_kernel(
    n_row, w_ref, g_ref, t_ref, p_ref,
    w_in, g_in, w_sum, g_sum, w_full, g_full, send_1, recv_1, send_2, recv_2,
):
    r = lax.axis_index("row")
    c = lax.axis_index("col")
    barrier = pltpu.get_barrier_semaphore()
    for d in range(1, n_row):
        pl.semaphore_signal(barrier, inc=1, device_id=(r ^ d, c), device_id_type=MESH)
    pl.semaphore_wait(barrier, n_row - 1)
    pairs = ((w_ref, w_in, w_sum, w_full), (g_ref, g_in, g_sum, g_full))

    def part(array, owner):
        size = array.shape[0] // n_row
        return pl.ds(pl.multiple_of(owner * size, size), size)

    def scatter(d, i):
        array, landing, _, _ = pairs[i]
        return pltpu.make_async_remote_copy(
            src_ref=array.at[part(array, r ^ d), :], dst_ref=landing.at[d],
            send_sem=send_1.at[d, i], recv_sem=recv_1.at[d, i],
            device_id=(r ^ d, c), device_id_type=MESH,
        )

    def spread(d, i):
        array, _, total, full = pairs[i]
        return pltpu.make_async_remote_copy(
            src_ref=total, dst_ref=full.at[part(array, r), :],
            send_sem=send_2.at[d, i], recv_sem=recv_2.at[d, i],
            device_id=(r ^ d, c), device_id_type=MESH,
        )

    every = [(d, i) for d in range(1, n_row) for i in (1, 0)]
    for d, i in every:
        scatter(d, i).start()
    for d, i in every:
        scatter(d, i).wait_recv()
    for i in (1, 0):
        array, landing, total, full = pairs[i]
        value = array[part(array, r), :]
        for d in range(1, n_row):
            value = value + landing[d]
        total[...] = value
    for i in (1, 0):
        array, _, total, full = pairs[i]
        full[part(array, r), :] = total[...]
    for d, i in every:
        spread(d, i).start()
    for d, i in every:
        spread(d, i).wait_recv()
    highest = lax.Precision.HIGHEST
    width = g_ref.shape[0]
    second = jnp.dot(
        t_ref[1], w_full[width:, :], precision=highest, preferred_element_type=jnp.float32
    ).astype(jnp.bfloat16)
    first = w_full[:width, :] - jnp.dot(
        g_full[...], second.astype(jnp.float32),
        precision=highest, preferred_element_type=jnp.float32,
    )
    first = jnp.dot(t_ref[0], first, precision=highest, preferred_element_type=jnp.float32)
    p_ref[0] = first.astype(jnp.bfloat16)
    p_ref[1] = second
    for d, i in every:
        scatter(d, i).wait_send()
        spread(d, i).wait_send()


def project(w, g, factors, n_row):
    dma = pltpu.SemaphoreType.DMA((n_row, 2))
    width, columns = g.shape[0], w.shape[1]
    vmem = pl.BlockSpec(memory_space=pltpu.VMEM)

    def landing(array):
        return pltpu.VMEM((n_row, array.shape[0] // n_row, array.shape[1]), jnp.float32)

    def total(array):
        return pltpu.VMEM((array.shape[0] // n_row, array.shape[1]), jnp.float32)

    return pl.pallas_call(
        functools.partial(project_kernel, n_row),
        out_shape=jax.ShapeDtypeStruct((2, width, columns), jnp.bfloat16),
        in_specs=[vmem] * 3,
        out_specs=vmem,
        scratch_shapes=[
            landing(w), landing(g), total(w), total(g),
            pltpu.VMEM(w.shape, jnp.float32), pltpu.VMEM(g.shape, jnp.float32),
            dma, dma, dma, dma,
        ],
        compiler_params=pltpu.CompilerParams(collective_id=1, has_side_effects=True),
        name="project",
    )(w, g, factors)


def region_kernel(index_ref, p_ref, vecs_ref, refl_ref, out_ref, vecs, refl, sems):
    count = vecs.shape[0]

    def copies(b):
        at = index_ref[b]
        return (
            pltpu.make_async_copy(vecs_ref.at[at], vecs.at[b], sems.at[b, 0]),
            pltpu.make_async_copy(refl_ref.at[0, at], refl.at[0, b], sems.at[b, 1]),
            pltpu.make_async_copy(refl_ref.at[1, at], refl.at[1, b], sems.at[b, 2]),
        )

    for b in range(count):
        for copy in copies(b):
            copy.start()
    for b in range(count):
        for copy in copies(b):
            copy.wait()
        value = vecs[b].astype(jnp.float32)
        value = value - jnp.dot(refl[1, b], p_ref[1], preferred_element_type=jnp.float32)
        value = value - jnp.dot(refl[0, b], p_ref[0], preferred_element_type=jnp.float32)
        out_ref[b] = value.astype(out_ref.dtype)


def region_rows(index, applied, vecs, refl):
    count = index.shape[0]
    columns, width = vecs.shape[2], refl.shape[3]
    vmem = pl.BlockSpec(memory_space=pltpu.VMEM)
    hbm = pl.BlockSpec(memory_space=pl.ANY)
    return pl.pallas_call(
        region_kernel,
        out_shape=jax.ShapeDtypeStruct((count, BLOCK, columns), vecs.dtype),
        in_specs=[pl.BlockSpec(memory_space=pltpu.SMEM), vmem, hbm, hbm],
        out_specs=vmem,
        scratch_shapes=[
            pltpu.VMEM((count, BLOCK, columns), vecs.dtype),
            pltpu.VMEM((2, count, BLOCK, width), refl.dtype),
            pltpu.SemaphoreType.DMA((count, 3)),
        ],
        name="region",
    )(index, applied, vecs, refl)


def per_device(n_row, eigvecs, reflectors, factors, frequencies, region_blocks):
    columns = eigvecs.shape[1]
    width = reflectors.shape[2]
    local = lax.dot_general(
        reflectors, eigvecs, (((1,), (0,)), ((), ())), preferred_element_type=jnp.float32
    ).reshape(2 * width, columns)
    cross_local = contract_rows(reflectors[0], reflectors[1])
    applied = project(local, cross_local, jnp.triu(factors), n_row)
    local_blocks = eigvecs.shape[0] // BLOCK
    local_index = region_blocks - lax.axis_index("row") * local_blocks
    region = region_rows(
        local_index,
        applied,
        eigvecs.reshape(local_blocks, BLOCK, columns),
        reflectors.reshape(2, local_blocks, BLOCK, width),
    ).reshape(-1, columns)
    weight = 1.0 / jnp.tanh(frequencies / 2.0) / (2.0 * frequencies)
    mine, partner = exchange(region, n_row)
    scaled = (mine.astype(jnp.float32) * weight[None, :]).astype(jnp.bfloat16)
    return contract_cols(scaled, partner)


def solution(mesh):
    return jax.shard_map(
        functools.partial(per_device, mesh.shape["row"]),
        mesh=mesh,
        in_specs=(P("row", "col"), P(None, "row", None), P(), P(), P("row")),
        out_specs=P("row", "col"),
        check_vma=False,
    )
```
